128 devices in a mesh: layer: 8 (over z, x_lo), tok: 16 (over x_hi, y, core).
Axes of the slice: x: 4 (x_hi: 2, x_lo: 2; x = x_hi * 2 + x_lo), y: 4, z: 4, core: 2. Of those that a mesh axis runs over, the one named last changes fastest.
Arguments:
- acts: bfloat16 [8, 32768, 4096], P('layer', 'tok'), may hold values from -48 to 48
- probe_weight: bfloat16 [8, 4096, 512], P('layer'), may hold values from -0.09375 to 0.09375
- mix_table: int32 [16, 2], replicated, may hold values from 0 to 7
- mix_scale: float32 [16], replicated, may hold values from 0.1 to 0.4
- labels: int32 [32768], P('tok'), may hold values from 0 to 511
Outputs:
- probe_grad: float32 [8, 4096, 512], P('layer', 'tok')
The draws below stay inside these ranges and needn't reach their ends.
All inputs are finite; a program needn't handle non-finite values.
Results may differ from the reference program's by a relative error of at most 0.0028.
Values may be sent and summed in bfloat16 or wider, within the bound.
No kernel may reach another device: no remote copies, remote signals or barrier semaphores. Data moves between devices by JAX's collectives and lax.ppermute only.
A program may use at most 256 MiB of HBM per device.

```python
import math
import jax
import jax.numpy as jnp
from jax import lax

D = 4096
CLASSES = 512
PAIRS = 16
LAYERS = 8
TOKENS = 32768


def draw_acts(key, part):
    first = jax.random.fold_in(jax.random.fold_in(key, 11), 0)
    values = jax.random.truncated_normal(first, -6.0, 6.0, (LAYERS, TOKENS, D), jnp.float32)
    return values.astype(jnp.bfloat16)


def set_ends(drawn, stream_key, smallest, high):
    longest = drawn.shape.index(max(drawn.shape))
    spots = []
    for shift in (0, 1):
        where = [jax.random.randint(jax.random.fold_in(stream_key, axis), (), 0, length) for axis, length in enumerate(drawn.shape)]
        where[longest] = (where[longest] + shift) % drawn.shape[longest]
        spots.append(tuple(where))
    return drawn.at[spots[0]].set(smallest).at[spots[1]].set(high)


def block_levels(rng, shape, cuts, least, top_value):
    def one(axis_at, blocks):
        heights = jax.random.uniform(jax.random.fold_in(jax.random.fold_in(rng, 6), axis_at), (blocks,), jnp.float32, least / len(cuts), top_value / len(cuts))
        return jnp.repeat(jnp.exp(heights), shape[axis_at] // blocks).reshape((-1,) + (1,) * (len(shape) - axis_at - 1))

    level = one(*cuts[0])
    for cut in cuts[1:]:
        level = level * one(*cut)
    return level


def centred(rng, dims, width, reach, cuts=(), kind=jnp.bfloat16):
    factor_of = block_levels(rng, dims, cuts, -0.22, 0.18) if cuts else 1.0
    entries = jax.random.normal(rng, dims, jnp.float32) * width * factor_of
    return jnp.minimum(jnp.maximum(entries, -reach), reach).astype(kind)


def setup_inputs(seed: int = 0) -> dict:
    arg_keys = jax.random.split(jax.random.key(seed), 6)
    acts = draw_acts(jax.random.fold_in(arg_keys[5], 71), 0)
    probe_weight = centred(arg_keys[1], (LAYERS, D, CLASSES), D ** -0.5, 0.09375, ((0, 8),))
    mix_table = set_ends(jax.random.randint(arg_keys[2], (PAIRS, 2), 0, LAYERS), jax.random.fold_in(arg_keys[2], 1), 0, LAYERS - 1).astype(jnp.int32)
    mix_scale = jnp.clip(jnp.exp(jax.random.uniform(arg_keys[3], (PAIRS,), jnp.float32, math.log(0.1), math.log(0.4))), 0.1, 0.4)
    labels = set_ends(jax.random.randint(arg_keys[4], (TOKENS,), 0, CLASSES), jax.random.fold_in(arg_keys[4], 1), 0, CLASSES - 1).astype(jnp.int32)
    return dict(acts=acts, probe_weight=probe_weight, mix_table=mix_table, mix_scale=mix_scale, labels=labels)


def loss_grad(partial_value, labels, pick_a, pick_b, mix_scale, norm):
    classes = partial_value.shape[2]
    wide = partial_value.astype(jnp.float32)
    best = lax.Precision.HIGHEST
    first = jnp.einsum('ql,lnc->qnc', pick_a, wide, precision=best)
    second = jnp.einsum('ql,lnc->qnc', pick_b, wide, precision=best)
    logits = lax.optimization_barrier(jnp.sum(wide, axis=0)) + jnp.einsum('q,qnc->nc', mix_scale, first * second, precision=best)
    top = lax.optimization_barrier(jnp.max(logits, axis=1, keepdims=True))
    expo = jnp.exp(logits - top)
    probs = expo / lax.optimization_barrier(jnp.sum(expo, axis=1, keepdims=True))
    onehot = (labels[:, None] == jnp.arange(classes, dtype=jnp.int32)[None, :]).astype(jnp.float32)
    grad = (probs - onehot) * norm
    weighted_a = pick_a * mix_scale[:, None]
    weighted_b = pick_b * mix_scale[:, None]
    factor = jnp.einsum('ql,qnc->lnc', weighted_a, second, precision=best) + jnp.einsum('ql,qnc->lnc', weighted_b, first, precision=best)
    return (grad[None] * (1.0 + factor)).astype(jnp.bfloat16)

def reference(acts, probe_weight, mix_table, mix_scale, labels):
    layers = acts.shape[0]
    span = jnp.arange(layers, dtype=jnp.int32)[None, :]
    pick_a = (mix_table[:, 0:1] == span).astype(jnp.float32)
    pick_b = (mix_table[:, 1:2] == span).astype(jnp.float32)
    scale = mix_scale.astype(jnp.float32)

    def project(pair):
        return jnp.dot(pair[0], pair[1], preferred_element_type=jnp.float32)
    partial_value = lax.map(project, (acts, probe_weight))
    block = math.gcd(TOKENS, 512)
    count = TOKENS // block
    blocks = partial_value.reshape(layers, count, block, CLASSES).transpose(1, 0, 2, 3)
    label_blocks = labels.reshape(count, block)
    norm = 1.0 / math.sqrt(TOKENS)

    def one_block(pair):
        return loss_grad(pair[0], pair[1], pick_a, pick_b, scale, norm)
    dpartial = lax.map(one_block, (blocks, label_blocks))
    dpartial = dpartial.transpose(1, 0, 2, 3).reshape(layers, TOKENS, CLASSES)

    def weight_grad(pair):
        return jnp.dot(pair[0].T, pair[1], preferred_element_type=jnp.float32)
    return lax.map(weight_grad, (acts, dpartial))
```

```python
import functools
import math

import jax
import jax.numpy as jnp
from jax import lax
from jax.experimental import pallas as pl
from jax.experimental.pallas import tpu as pltpu
from jax.sharding import Mesh
from jax.sharding import PartitionSpec as P

LAYER = ("z", "xl")
CHIPS = ("xh", "y")
TOK = ("xh", "y", "core")
CHUNKS = 2
SEND = jnp.float32
ROWS = 512
MIB = 1024 * 1024


def params(mib):
    return pltpu.CompilerParams(vmem_limit_bytes=mib * MIB)


def whole(shape):
    return pl.BlockSpec(shape, lambda *_: (0,) * len(shape))


def partner(at, offset, long):
    if long == "first":
        return (at // 2 + offset // 2) % 4 * 2 + (at % 2 + offset % 2) % 2
    return (at // 4 + offset // 4) % 2 * 4 + (at % 4 + offset % 4) % 4


def routes(offset, long):
    return [(at, partner(at, offset, long)) for at in range(8)]


def back(pairs):
    return [(b, a) for a, b in pairs]


def members(at, sign):
    offset = jnp.arange(8, dtype=jnp.int32)
    return ((at >> 1) + sign * (offset >> 1) & 3) * 2 + ((at ^ offset) & 1)


def chips_at(at):
    offset = jnp.arange(8, dtype=jnp.int32)
    return ((at ^ offset) & 4) + (at + offset & 3)


def project_body(slot_ref, acts_ref, weight_ref, *refs):
    *outs, keep_ref = refs
    rows = outs[0].shape[0]
    step = pl.program_id(0)
    value = jnp.dot(acts_ref[0], weight_ref[0], preferred_element_type=jnp.float32)
    count = value.shape[0] // rows
    for m in range(count):
        keep_ref[slot_ref[step * count + m]] = value[m * rows : (m + 1) * rows].astype(keep_ref.dtype)

    @pl.when(step == pl.num_programs(0) - 1)
    def _():
        for slot, out_ref in enumerate(outs):
            out_ref[...] = keep_ref[slot]


def project(slots, acts, weight, chunk, chunks, groups):
    _, tokens, width = acts.shape
    classes = weight.shape[2]
    size = tokens // chunks
    block = min(ROWS, size)
    first = chunk * size // block
    rows = size // groups
    return pl.pallas_call(
        project_body,
        grid_spec=pltpu.PrefetchScalarGridSpec(
            num_scalar_prefetch=1,
            grid=(size // block,),
            in_specs=[
                pl.BlockSpec((1, block, width), lambda i, _: (0, first + i, 0)),
                whole((1, width, classes)),
            ],
            out_specs=[whole((rows, classes))] * groups,
            scratch_shapes=[pltpu.VMEM((groups, rows, classes), SEND)],
        ),
        out_shape=[jax.ShapeDtypeStruct((rows, classes), SEND)] * groups,
        compiler_params=params(26),
        cost_estimate=pl.CostEstimate(
            flops=2 * size * width * classes,
            bytes_accessed=2 * size * width + 2 * width * classes + 4 * size * classes,
            transcendentals=0,
        ),
        name=f"project{chunk}",
    )(slots, acts, weight)


def score_body(mix_ref, label_ref, *refs, norm, step, layers):
    parts = refs[:layers]
    outs = refs[layers : 2 * layers]
    keep_ref = refs[2 * layers]
    rows, classes = parts[0].shape
    lane = lax.broadcasted_iota(jnp.int32, (step, classes), 1)

    def one(i, carry):
        at = pl.ds(pl.multiple_of(i * step, step), step)
        part = [ref[at, :].astype(jnp.float32) for ref in parts]
        logits = None
        for l in range(layers):
            factor = mix_ref[l * layers] * part[0]
            for b in range(1, layers):
                factor = factor + mix_ref[l * layers + b] * part[b]
            keep_ref[l, at, :] = 1.0 + factor
            term = part[l] * (1.0 + 0.5 * factor)
            logits = term if logits is None else logits + term
        top = jnp.max(logits, axis=1, keepdims=True)
        expo = jnp.exp(logits - top)
        probs = expo / jnp.sum(expo, axis=1, keepdims=True)
        hot = (lane == label_ref[at, :]).astype(jnp.float32)
        grad = (probs - hot) * norm
        for l in range(layers):
            keep_ref[l, at, :] = grad * keep_ref[l, at, :]
        return carry

    lax.fori_loop(0, rows // step, one, 0)
    for l in range(layers):
        outs[l][...] = keep_ref[l].T.astype(outs[l].dtype)


def score(mix, labels, parts, norm, chunk):
    layers = len(parts)
    rows, classes = parts[0].shape
    return pl.pallas_call(
        functools.partial(score_body, norm=norm, step=8, layers=layers),
        in_specs=[pl.BlockSpec(memory_space=pltpu.SMEM), pl.BlockSpec()]
        + [pl.BlockSpec()] * layers,
        out_shape=[jax.ShapeDtypeStruct((classes, rows), jnp.bfloat16)] * layers,
        scratch_shapes=[pltpu.VMEM((layers, rows, classes), jnp.float32)],
        compiler_params=params(16),
        cost_estimate=pl.CostEstimate(
            flops=300 * rows * classes * layers,
            bytes_accessed=6 * rows * classes * layers,
            transcendentals=rows * classes,
        ),
        name=f"score{chunk}",
    )(mix, labels, *parts)


def weigh_body(cols_ref, slot_ref, acts_ref, *refs, grads, outs, adds):
    del cols_ref
    grad_refs = refs[:grads]
    refs = refs[grads:]
    if adds:
        add_ref, *refs = refs
    out_refs = refs[:outs]
    all_ref = refs[outs]
    step = pl.program_id(0)
    rows = grad_refs[0].shape[1]

    @pl.when(step == 0)
    def _():
        for k, ref in enumerate(grad_refs):
            at = pl.multiple_of(slot_ref[k] * rows, rows)
            all_ref[:, pl.ds(at, rows)] = ref[...]

    total = jnp.dot(all_ref[...], acts_ref[0], preferred_element_type=jnp.float32)
    if not adds:
        out_refs[0][0] = total
        return
    total = total + add_ref[0]
    for k, out_ref in enumerate(out_refs):

        @pl.when(step == k)
        def _(out_ref=out_ref):
            out_ref[...] = total.astype(out_ref.dtype)


def weigh(blocks, slots, acts, grads, count, name, add=None, kinds=()):
    _, tokens, width = acts.shape
    classes = grads[0].shape[0]
    cols = width // 16
    in_specs = [pl.BlockSpec((1, tokens, cols), lambda j, blk, _: (0, 0, blk[j]))]
    in_specs += [whole(g.shape) for g in grads]
    operands = [acts, *grads]
    if add is None:
        out_specs = [pl.BlockSpec((1, classes, cols), lambda j, *_: (j, 0, 0))]
        out_shape = [jax.ShapeDtypeStruct((count, classes, cols), jnp.float32)]
    else:
        in_specs.append(pl.BlockSpec((1, classes, cols), lambda j, *_: (j, 0, 0)))
        operands.append(add)
        out_specs = [whole((classes, cols))] * count
        out_shape = [jax.ShapeDtypeStruct((classes, cols), kind) for kind in kinds]
    return pl.pallas_call(
        functools.partial(weigh_body, grads=len(grads), outs=len(out_shape), adds=add is not None),
        grid_spec=pltpu.PrefetchScalarGridSpec(
            num_scalar_prefetch=2,
            grid=(count,),
            in_specs=in_specs,
            out_specs=out_specs,
            scratch_shapes=[pltpu.VMEM((classes, tokens), jnp.bfloat16)],
        ),
        out_shape=out_shape,
        compiler_params=params(26),
        cost_estimate=pl.CostEstimate(
            flops=2 * tokens * cols * classes * count,
            bytes_accessed=2 * tokens * cols * count + 2 * tokens * classes + 4 * count * cols * classes,
            transcendentals=0,
        ),
        name=name,
    )(blocks, slots, *operands)


def merge_body(*refs):
    *got, out_ref = refs
    total = got[0][...].astype(jnp.float32)
    for ref in got[1:]:
        total = total + ref[...].astype(jnp.float32)
    out_ref[0] = total.T


def merge(got):
    classes, cols = got[0].shape
    return pl.pallas_call(
        merge_body,
        out_shape=jax.ShapeDtypeStruct((1, cols, classes), jnp.float32),
        compiler_params=params(8),
        name="merge",
    )(*got)


def local(acts, probe_weight, mix_table, mix_scale, labels):
    _, tokens, width = acts.shape
    groups = lax.axis_size(LAYER)
    norm = 1.0 / math.sqrt(tokens * lax.axis_size(TOK))
    acts = pltpu.with_memory_space_constraint(acts, pltpu.HBM)
    probe_weight = pltpu.with_memory_space_constraint(probe_weight, pltpu.HBM)
    here = lax.axis_index(LAYER)
    chip = lax.axis_index(CHIPS)
    core = lax.axis_index("core")
    rows = tokens // CHUNKS // groups

    origin = members(here, -1)
    paired = (mix_table[:, 0, None, None] == origin[None, :, None]) & (
        mix_table[:, 1, None, None] == origin[None, None, :]
    )
    pairs = jnp.sum(jnp.where(paired, mix_scale[:, None, None], 0.0), axis=0)
    mix = (pairs + pairs.T).reshape(groups * groups)
    own = lax.dynamic_slice_in_dim(labels.reshape(CHUNKS, groups, rows), here, 1, 1)
    own = own.reshape(CHUNKS, rows, 1)

    span = jnp.arange(groups, dtype=jnp.int32)
    target = members(here, 1)
    slots = jnp.sum(jnp.where(target[:, None] == span[None, :], span[:, None], 0), axis=0)

    arrived = []
    for k in range(CHUNKS):
        parts = project(slots, acts, probe_weight, k, CHUNKS, groups)
        arrived.append(
            [parts[0]]
            + [lax.ppermute(parts[o], LAYER, routes(o, "first")) for o in range(1, groups)]
        )
    returned = []
    for k in range(CHUNKS):
        dparts = score(mix, own[k], arrived[k], norm, k)
        returned.append(
            [dparts[0]]
            + [lax.ppermute(dparts[o], LAYER, back(routes(o, "first"))) for o in range(1, groups)]
        )
    grads = [g for chunk in returned for g in chunk]
    place = (jnp.arange(CHUNKS, dtype=jnp.int32)[:, None] * groups + target[None, :]).reshape(-1)

    sides = ((1, 2, 3, 4), (5, 6, 7, 0))
    ahead = jnp.roll(chips_at(chip), -1)
    reach = [ahead[:4], ahead[4:]]
    swapped = []
    for s, side in enumerate(sides):
        (away,) = weigh(reach[s] * 2 + 1 - core, place, acts, grads, len(side), f"away{s}")
        swapped.append(lax.ppermute(away, "core", [(0, 1), (1, 0)]))
    got = []
    for s, side in enumerate(sides):
        kinds = [jnp.float32 if o == 0 else jnp.bfloat16 for o in side]
        mine = weigh(
            reach[s] * 2 + core, place, acts, grads, len(side), f"mine{s}", swapped[s], kinds
        )
        for o, piece in zip(side, mine, strict=True):
            got.append(lax.ppermute(piece, CHIPS, routes(o, "second")) if o else piece)
    return merge(got)


def solution(mesh):
    fine = Mesh(mesh.devices.reshape(4, 2, 2, 4, 2), ("z", "xl", "xh", "y", "core"))
    in_specs = (P(LAYER, TOK, None), P(LAYER, None, None), P(), P(), P(TOK))
    out_specs = P(LAYER, TOK, None)
    return jax.shard_map(local, mesh=fine, in_specs=in_specs, out_specs=out_specs, check_vma=False)
```

```python
import functools
import math

import jax
import jax.numpy as jnp
from jax import lax
from jax.experimental import pallas as pl
from jax.experimental.pallas import tpu as pltpu
from jax.sharding import Mesh
from jax.sharding import PartitionSpec as P


LAYER = ("z", "xl")
CHIPS = ("xh", "y")
TOK = ("xh", "y", "core")
CHUNKS = 2
NARROW = jnp.float16
PEAK = 8.0
PULL = 32.0
SCORE_STEP = 16
DEPTH = 4
AHEAD = 2
SIDES = ((6, 5, 7, 4), (2, 1, 3, 0))
MIB = 1024 * 1024


def params(mib):
    return pltpu.CompilerParams(vmem_limit_bytes=mib * MIB)


def whole(shape):
    return pl.BlockSpec(shape, lambda *_: (0,) * len(shape))


def partner(at, offset, long):
    if long == "first":
        return (at // 2 + offset // 2) % 4 * 2 + (at % 2 + offset % 2) % 2
    return (at // 4 + offset // 4) % 2 * 4 + (at % 4 + offset % 4) % 4


def routes(offset, long):
    return [(at, partner(at, offset, long)) for at in range(8)]


def back(pairs):
    return [(b, a) for a, b in pairs]


def member(at, offset, sign):
    return (((at >> 1) + sign * (offset >> 1)) & 3) * 2 + ((at ^ offset) & 1)


def chip_at(at, offset):
    return ((at ^ offset) & 4) + ((at + offset) & 3)


def project_body(ids_ref, table_ref, scale_ref, acts_ref, weight_ref, *refs, chunk, split, mark):
    outs = refs[:split]
    keep_ref, weight_vmem, acts_vmem, weight_sem, acts_sem = refs[split:]
    count, size, deep = acts_vmem.shape
    rows = size // split

    def fetch(k):
        at = pl.ds(k * deep, deep)
        half = size // 2
        return [
            pltpu.make_async_copy(weight_ref.at[0, at], weight_vmem.at[k], weight_sem.at[k])
        ] + [
            pltpu.make_async_copy(
                acts_ref.at[0, pl.ds(chunk * size + h * half, half), at],
                acts_vmem.at[k, pl.ds(h * half, half)],
                acts_sem.at[k, h],
            )
            for h in range(2)
        ]

    loads = [fetch(k) for k in range(count)]
    for k in range(AHEAD):
        for copy in loads[k]:
            copy.start()
    if mark:
        pairs = table_ref.shape[1]
        strength = 0.0
        for l in range(8):
            pull = 0.0
            for q in range(pairs):
                pull = pull + jnp.where(table_ref[0, q] == l, scale_ref[q], 0.0)
                pull = pull + jnp.where(table_ref[1, q] == l, scale_ref[q], 0.0)
            strength = jnp.maximum(strength, pull)
    for k in range(count):
        for copy in loads[k]:
            copy.wait()
        if k + AHEAD < count:
            for copy in loads[k + AHEAD]:
                copy.start()
        value = jnp.dot(acts_vmem[k], weight_vmem[k], preferred_element_type=jnp.float32)
        value = value if k == 0 else keep_ref[...] + value
        keep_ref[...] = value
    wide = False
    if mark:
        peak = jnp.max(jnp.abs(value))
        wide = (peak > PEAK) | (peak * strength > PULL)
    for slot, out_ref in enumerate(outs):
        at = pl.multiple_of(member(ids_ref[0], slot, 1) * rows, rows) if split > 1 else 0
        value = keep_ref[pl.ds(at, rows), :]
        out_ref[...] = jnp.where(wide, jnp.inf, value) if mark else value


def project(ids, table, scale, acts, weight, chunk, split, mark=True):
    _, tokens, width = acts.shape
    classes = weight.shape[2]
    size = tokens // CHUNKS
    piece = (size // split, classes)
    return pl.pallas_call(
        functools.partial(project_body, chunk=chunk, split=split, mark=mark),
        in_specs=[pl.BlockSpec(memory_space=pltpu.SMEM)] * 3
        + [pl.BlockSpec(memory_space=pl.ANY)] * 2,
        out_shape=[jax.ShapeDtypeStruct(piece, jnp.float32)] * split,
        scratch_shapes=[
            pltpu.VMEM((size, classes), jnp.float32),
            pltpu.VMEM((DEPTH, width // DEPTH, classes), weight.dtype),
            pltpu.VMEM((DEPTH, size, width // DEPTH), acts.dtype),
            pltpu.SemaphoreType.DMA((DEPTH,)),
            pltpu.SemaphoreType.DMA((DEPTH, 2)),
        ],
        compiler_params=params(22),
        cost_estimate=pl.CostEstimate(
            flops=2 * size * width * classes,
            bytes_accessed=2 * size * width + 2 * width * classes + 4 * size * classes,
            transcendentals=0,
        ),
    )(ids, table, scale, acts, weight)


def planes(refs):
    return [refs[0].at[l] for l in range(refs[0].shape[0])] if len(refs) == 1 else list(refs)


def score_body(ids_ref, table_ref, scale_ref, label_ref, *refs, norm, step, count, layers, chunk):
    parts = planes(refs[:count])
    outs = planes(refs[count : 2 * count])
    mark_ref, keep_ref, total_ref, mix_ref = refs[2 * count :]
    rows, classes = parts[0].shape
    here = ids_ref[0]
    for k in range(layers * layers):
        mix_ref[k] = 0.0
    for q in range(table_ref.shape[1]):
        left = table_ref[0, q]
        right = table_ref[1, q]
        if count > 1:
            left = member(here, left, -1)
            right = member(here, right, -1)
        mix_ref[left * layers + right] = mix_ref[left * layers + right] + scale_ref[q]
        mix_ref[right * layers + left] = mix_ref[right * layers + left] + scale_ref[q]
    most = parts[0][:8, :128]
    for ref in parts[1:]:
        most = jnp.maximum(most, ref[:8, :128])
    mark_ref[0] = jnp.max(most)

    def one(i, carry):
        at = pl.ds(pl.multiple_of(i * step, step), step)
        part = [ref[at, :].astype(jnp.float32) for ref in parts]
        logits = None
        for l in range(layers):
            factor = mix_ref[l * layers] * part[0]
            for b in range(1, layers):
                factor = factor + mix_ref[l * layers + b] * part[b]
            keep_ref[l, at, :] = 1.0 + factor
            term = part[l] * (1.0 + 0.5 * factor)
            logits = term if logits is None else logits + term
        total_ref[at, :] = logits
        return carry

    lax.fori_loop(0, rows // step, one, 0)
    lane = lax.broadcasted_iota(jnp.int32, (rows, classes), 1)
    logits = total_ref[...]
    top = jnp.max(logits, axis=1, keepdims=True)
    expo = jnp.exp(logits - top)
    probs = expo / jnp.sum(expo, axis=1, keepdims=True)
    label = label_ref[pl.ds(chunk * layers + here, 1), :]
    label = jnp.broadcast_to(label, (8, rows)).T[:, :1]
    hot = (lane == label).astype(jnp.float32)
    total_ref[...] = (probs - hot) * norm
    for l in range(layers):
        outs[l][...] = (total_ref[...] * keep_ref[l]).astype(jnp.bfloat16)


def score(ids, table, scale, labels, parts, norm, chunk):
    if len(parts) == 1:
        layers, rows, classes = parts[0].shape
        out_shape = [jax.ShapeDtypeStruct((layers, rows, classes), jnp.bfloat16)]
    else:
        layers = len(parts)
        rows, classes = parts[0].shape
        out_shape = [jax.ShapeDtypeStruct((rows, classes), jnp.bfloat16)] * layers
    return pl.pallas_call(
        functools.partial(
            score_body,
            norm=norm,
            step=SCORE_STEP,
            count=len(parts),
            layers=layers,
            chunk=chunk,
        ),
        in_specs=[pl.BlockSpec(memory_space=pltpu.SMEM)] * 3
        + [pl.BlockSpec()] * (1 + len(parts)),
        out_specs=[pl.BlockSpec()] * len(parts) + [pl.BlockSpec(memory_space=pltpu.SMEM)],
        out_shape=out_shape + [jax.ShapeDtypeStruct((1,), jnp.float32)],
        scratch_shapes=[
            pltpu.VMEM((layers, rows, classes), jnp.float32),
            pltpu.VMEM((rows, classes), jnp.float32),
            pltpu.SMEM((layers * layers,), jnp.float32),
        ],
        compiler_params=params(16),
        cost_estimate=pl.CostEstimate(
            flops=300 * rows * classes * layers,
            bytes_accessed=6 * rows * classes * layers,
            transcendentals=rows * classes,
        ),
    )(ids, table, scale, labels, *parts)


def gather_body(ids_ref, *refs):
    *grads, out_ref = refs
    rows = out_ref.shape[0] // 16
    pieces = [piece for ref in grads for piece in (planes([ref]) if len(ref.shape) == 3 else [ref])]
    for k, ref in enumerate(pieces):
        slot = 8 + member(ids_ref[0], k - 8, 1) if len(grads) > 2 and k >= 8 else k
        out_ref[pl.ds(slot * rows, rows), :] = ref[...]


def gather(ids, grads, tokens):
    classes = grads[0].shape[-1]
    return pl.pallas_call(
        gather_body,
        in_specs=[pl.BlockSpec(memory_space=pltpu.SMEM)] + [pl.BlockSpec()] * len(grads),
        out_shape=jax.ShapeDtypeStruct((tokens, classes), jnp.bfloat16),
        compiler_params=params(12),
        cost_estimate=pl.CostEstimate(
            flops=tokens * classes, bytes_accessed=4 * tokens * classes, transcendentals=0
        ),
    )(ids, *grads)


def weigh_body(ids_ref, acts_ref, grad_ref, away_ref, mine_ref, acts_vmem, sem, *, offsets):
    step = pl.program_id(0)
    _, tokens, wide = acts_vmem.shape
    parts = sem.shape[2]
    tall = tokens // parts
    cols = wide // 2
    core = ids_ref[2]

    def fetch(j, side, r, block):
        return pltpu.make_async_copy(
            acts_ref.at[0, pl.ds(r * tall, tall), pl.ds(pl.multiple_of(block * cols, cols), cols)],
            acts_vmem.at[j, pl.ds(r * tall, tall), pl.ds(side * cols, cols)],
            sem.at[j, side, r],
        )

    @pl.when(step == 0)
    def _():
        for j, offset in enumerate(offsets):
            block = chip_at(ids_ref[1], offset) * 2 + core
            for side in range(2):
                for r in range(parts):
                    fetch(j, side, r, block ^ side).start()

    for side in range(2):
        for r in range(parts):
            fetch(step, side, r, 0).wait()
    total = lax.dot_general(
        acts_vmem[step],
        grad_ref[...],
        (((0,), (0,)), ((), ())),
        preferred_element_type=jnp.float32,
    )
    mine_ref[0] = total[:cols]
    away_ref[0] = total[cols:]


def weigh(ids, offsets, acts, grads):
    _, tokens, width = acts.shape
    classes = grads.shape[1]
    wide = width // 8
    count = len(offsets)
    half = pl.BlockSpec((1, wide // 2, classes), lambda j: (j, 0, 0))
    return pl.pallas_call(
        functools.partial(weigh_body, offsets=offsets),
        grid=(count,),
        in_specs=[
            pl.BlockSpec(memory_space=pltpu.SMEM),
            pl.BlockSpec(memory_space=pl.ANY),
            whole(grads.shape),
        ],
        out_specs=[half, half],
        scratch_shapes=[
            pltpu.VMEM((count, tokens, wide), acts.dtype),
            pltpu.SemaphoreType.DMA((count, 2, 1)),
        ],
        out_shape=[jax.ShapeDtypeStruct((count, wide // 2, classes), jnp.float32)] * 2,
        compiler_params=params(22),
        cost_estimate=pl.CostEstimate(
            flops=2 * tokens * wide * classes * count,
            bytes_accessed=2 * tokens * wide * count + 2 * tokens * classes + 4 * count * wide * classes,
            transcendentals=0,
        ),
    )(ids, acts, grads)


def join_body(mine_ref, away_ref, *outs):
    for k, out_ref in enumerate(outs):
        out_ref[...] = (mine_ref[k] + away_ref[k]).astype(out_ref.dtype)


def join(mine, away, kinds):
    return pl.pallas_call(
        join_body,
        out_shape=[jax.ShapeDtypeStruct(mine.shape[1:], kind) for kind in kinds],
        compiler_params=params(12),
        cost_estimate=pl.CostEstimate(
            flops=2 * mine.size, bytes_accessed=10 * mine.size, transcendentals=0
        ),
    )(mine, away)


def merge_body(*refs):
    *got, out_ref = refs
    got = planes(got)
    total = got[0][...].astype(jnp.float32)
    for ref in got[1:]:
        total = total + ref[...].astype(jnp.float32)
    out_ref[0] = total


def merge(got):
    cols, classes = got[0].shape[-2:]
    return pl.pallas_call(
        merge_body,
        out_shape=jax.ShapeDtypeStruct((1, cols, classes), jnp.float32),
        compiler_params=params(8),
        name="merge",
    )(*got)


def local(acts, probe_weight, mix_table, mix_scale, labels):
    tokens = acts.shape[1]
    classes = probe_weight.shape[2]
    groups = lax.axis_size(LAYER)
    norm = 1.0 / math.sqrt(tokens * lax.axis_size(TOK))
    acts = pltpu.with_memory_space_constraint(acts, pltpu.HBM)
    probe_weight = pltpu.with_memory_space_constraint(probe_weight, pltpu.HBM)
    ids = jnp.stack([lax.axis_index(LAYER), lax.axis_index(CHIPS), lax.axis_index("core")])
    ids = ids.astype(jnp.int32)
    rows = tokens // CHUNKS // groups
    table = mix_table.T
    labels = labels.reshape(CHUNKS * groups, rows)
    mixing = (ids, table, mix_scale)

    (part0,) = project(*mixing, acts, probe_weight, 0, 1)
    part0 = part0.reshape(groups, rows, classes).astype(NARROW)
    arrived0 = lax.all_to_all(part0, LAYER, split_axis=0, concat_axis=0, tiled=True)
    part1 = project(*mixing, acts, probe_weight, 1, groups)
    first1 = part1[0]
    sent1 = []
    for o in range(1, groups):
        sent1.append(lax.ppermute(part1[o].astype(NARROW), LAYER, routes(o, "first")))
    wider0 = arrived0.astype(jnp.float32)
    dpart0, mark0 = score(*mixing, labels, [wider0], norm, 0)
    returned0 = lax.all_to_all(dpart0, LAYER, split_axis=0, concat_axis=0, tiled=True)
    arrived1 = [first1] + [s.astype(jnp.float32) for s in sent1]
    *dpart1, mark1 = score(*mixing, labels, arrived1, norm, 1)
    returned1 = [dpart1[0]]
    returned1 += [lax.ppermute(dpart1[o], LAYER, back(routes(o, "first"))) for o in range(1, groups)]
    wide = (mark0[0] == jnp.inf) | (mark1[0] == jnp.inf)

    def keep(returned0, *returned1):
        return gather(ids, [returned0, *returned1], tokens)

    def again(*_):
        returned = []
        for k in range(CHUNKS):
            (part,) = project(*mixing, acts, probe_weight, k, 1, False)
            arrived = lax.all_to_all(
                part.reshape(groups, rows, classes), LAYER, split_axis=0, concat_axis=0, tiled=True
            )
            dpart, _ = score(*mixing, labels, [arrived], norm, k)
            returned.append(lax.all_to_all(dpart, LAYER, split_axis=0, concat_axis=0, tiled=True))
        return gather(ids, returned, tokens)

    grads = lax.cond(wide, again, keep, returned0, *returned1)

    kept = []
    for side in SIDES:
        away, mine = weigh(ids, side, acts, grads)
        kept.append((mine, lax.ppermute(away, "core", [(0, 1), (1, 0)])))
    got = []
    for s, side in enumerate(SIDES):
        kinds = [jnp.float32 if o == 0 else jnp.bfloat16 for o in side]
        for o, piece in zip(side, join(*kept[s], kinds), strict=True):
            got.append(lax.ppermute(piece, CHIPS, routes(o, "second")) if o else piece)
    return merge(got)


def solution(mesh):
    fine = Mesh(mesh.devices.reshape(4, 2, 2, 4, 2), ("z", "xl", "xh", "y", "core"))
    in_specs = (P(LAYER, TOK, None), P(LAYER, None, None), P(), P(), P(TOK))
    out_specs = P(LAYER, TOK, None)
    return jax.shard_map(
        local, mesh=fine, in_specs=in_specs, out_specs=out_specs, check_vma=False
    )
```
